8 devices in a mesh: rep: 2 (over y, z), dp: 4 (over x, core).
Axes of the slice: x: 2, y: 2, z: 1, core: 2. Of those that a mesh axis runs over, the one named last changes fastest.
Arguments:
- a: bfloat16 [8, 4, 4096, 1280], P(('rep', 'dp')), parts along dimension 0
- g: bfloat16 [8, 4, 4096, 4096], P(('rep', 'dp')), parts along dimension 0
Outputs:
- output: bfloat16 [8, 1280, 4096], P('rep'), parts along dimension 0
There are 2 independent parts. The reference program is written for one: setup_inputs(seed, part) draws one part's arguments, and reference() takes and returns one part's arrays. A program takes and returns all parts, laid end to end along the dimension named above; each array names one.
All inputs are finite; a program needn't handle non-finite values.
Results may differ from the reference program's by a relative error of at most 0.012.
Values are sent between devices in bfloat16 or wider.
A program may use at most 2 GiB of HBM per device.

```python
import jax
import jax.numpy as jnp
from jax import lax

DEVICES = 4
MATRICES = 4
TOKENS = 4096
D = 1280
FF = 4096


def setup_inputs(seed: int = 0, part: int = 0) -> dict:
    ka, kg, ks = (jax.random.fold_in(k, part) for k in jax.random.split(jax.random.key(seed), 3))
    size = 2.0 ** jax.random.uniform(ks, (DEVICES, MATRICES, 1, 1), jnp.float32, -1.0, 1.0)
    a = jax.random.normal(ka, (DEVICES, MATRICES, TOKENS, D), jnp.float32)
    g = size * jax.random.normal(kg, (DEVICES, MATRICES, TOKENS, FF), jnp.float32) * (DEVICES * TOKENS) ** -0.5
    return {"a": a.astype(jnp.bfloat16), "g": g.astype(jnp.bfloat16)}


def reference(a, g):
    def take(so_far, one):
        return so_far + jnp.einsum("ntd,ntf->ndf", *one, preferred_element_type=jnp.float32), None

    return lax.scan(take, jnp.zeros((MATRICES, D, FF), jnp.float32), (a, g))[0].astype(jnp.bfloat16)
```

```python
import jax
import jax.numpy as jnp
from jax import lax
from jax.experimental import pallas as pl
from jax.experimental.pallas import tpu as pltpu
from jax.sharding import PartitionSpec as P

MESH = pl.DeviceIdType.MESH
N, TOK, D, FF = 4, 4096, 1280, 4096
RB, CB = 256, 512
HB = RB // 2
NR, NC = D // RB, FF // CB
PIECES = N * NC * NR
KT = 512
LAG = 24
QX = LAG + 2
QD = 4
QP = 3
QF = 4


def when(cond):
    return pl.when(cond)


def kernel(a, g, res, at, abuf, gbuf, prod, dsend, drecv, xsend, xrecv, fin,
           a_sem, g_sem, ds_sem, dr_sem, xs_sem, xr_sem, fl_sem, fs_sem, fr_sem,
           dfree, xfree):
    rep, me = lax.axis_index("rep"), lax.axis_index("dp")
    core = lax.rem(me, 2)
    sibling = (rep, me + 1 - 2 * core)
    partner = (rep, lax.rem(me + 2, 4))
    mine = pl.multiple_of(core * HB, HB)
    other = pl.multiple_of((1 - core) * HB, HB)

    def load_a(t):
        n, r = t // NR, lax.rem(t, NR)
        s = lax.rem(t, 2)
        cols = pl.ds(pl.multiple_of(r * RB, RB), RB)
        return pltpu.make_async_copy(a.at[n, :, cols], abuf.at[s], a_sem.at[s])

    def load_g(q):
        n, c = q // NC, lax.rem(q, NC)
        s = lax.rem(q, 2)
        cols = pl.ds(pl.multiple_of(c * CB, CB), CB)
        return pltpu.make_async_copy(g.at[n, :, cols], gbuf.at[s], g_sem.at[s])

    def across_cores(k):
        s = lax.rem(k, QD)
        return pltpu.make_async_remote_copy(
            dsend.at[s], drecv.at[s], ds_sem.at[s], dr_sem.at[s],
            device_id=sibling, device_id_type=MESH)

    def across_chips(k):
        s = lax.rem(k, QX)
        return pltpu.make_async_remote_copy(
            xsend.at[s], xrecv.at[s], xs_sem.at[s], xr_sem.at[s],
            device_id=partner, device_id_type=MESH)

    def place(k):
        q = k // NR
        n, c, r = q // NC, lax.rem(q, NC), lax.rem(k, NR)
        rows = pl.ds(pl.multiple_of(r * RB + mine, HB), HB)
        cols = pl.ds(pl.multiple_of(c * CB, CB), CB)
        return res.at[n, rows, cols]

    def keep(k):
        s = lax.rem(k, QF)
        return pltpu.make_async_copy(fin.at[s], place(k), fl_sem.at[s])

    def share(k):
        s = lax.rem(k, QF)
        return pltpu.make_async_remote_copy(
            fin.at[s], place(k), fs_sem.at[s], fr_sem,
            device_id=sibling, device_id_type=MESH)

    def multiply(k):
        q, r = k // NR, lax.rem(k, NR)
        n, c = q // NC, lax.rem(q, NC)
        gs = lax.rem(q, 2)

        @when(c == 0)
        def _():
            t = n * NR + r
            s = lax.rem(t, 2)
            load_a(t).wait()

            @pl.loop(0, TOK // KT)
            def _(i):
                toks = pl.ds(pl.multiple_of(i * KT, KT), KT)
                at[r, :, toks] = abuf[s, toks, :].T

            @when(t + 2 < N * NR)
            def _():
                load_a(t + 2).start()

        @when(r == 0)
        def _():
            load_g(q).wait()

        p = lax.rem(k, QP)
        prod[p] = jnp.dot(at[r], gbuf[gs], preferred_element_type=jnp.float32)

        @when((r == NR - 1) & (q + 2 < N * NC))
        def _():
            load_g(q + 2).start()

        @when(k >= QD)
        def _():
            across_cores(k - QD).wait_send()
            pl.semaphore_wait(dfree, 1)

        dsend[lax.rem(k, QD)] = prod[p, pl.ds(other, HB)].astype(jnp.bfloat16)
        across_cores(k).start()

    def chip_sum(k):
        across_cores(k).wait_recv()
        total = prod[lax.rem(k, QP), pl.ds(mine, HB)] + drecv[lax.rem(k, QD)].astype(jnp.float32)
        xsend[lax.rem(k, QX)] = total.astype(jnp.bfloat16)

        @when(k + QD < PIECES)
        def _():
            pl.semaphore_signal(dfree, inc=1, device_id=sibling, device_id_type=MESH)

        @when(k >= QX)
        def _():
            pl.semaphore_wait(xfree, 1)

        across_chips(k).start()

    def finish(k):
        across_chips(k).wait()

        @when(k >= QF)
        def _():
            keep(k - QF).wait()
            share(k - QF).wait_send()

        s = lax.rem(k, QX)
        total = xsend[s].astype(jnp.float32) + xrecv[s].astype(jnp.float32)
        fin[lax.rem(k, QF)] = total.astype(jnp.bfloat16)

        @when(k + QX < PIECES)
        def _():
            pl.semaphore_signal(xfree, inc=1, device_id=partner, device_id_type=MESH)

        keep(k).start()
        share(k).start()

    load_a(0).start()
    load_g(0).start()
    load_a(1).start()
    load_g(1).start()
    barrier = pltpu.get_barrier_semaphore()
    for peer in (sibling, partner):
        pl.semaphore_signal(barrier, inc=1, device_id=peer, device_id_type=MESH)
    pl.semaphore_wait(barrier, 2)

    @pl.loop(0, PIECES + LAG)
    def _(k):
        @when(k < PIECES)
        def _():
            multiply(k)

        @when((k != 1) & (k <= PIECES))
        def _():
            chip_sum(jnp.maximum(k - 1, 0))

        @when(k >= LAG)
        def _():
            finish(k - LAG)

    @pl.loop(PIECES - QD, PIECES)
    def _(k):
        across_cores(k).wait_send()

    @pl.loop(PIECES - QF, PIECES)
    def _(k):
        keep(k).wait()
        share(k).wait_send()

    half = res.at[pl.ds(0, N // 2)]
    pltpu.make_async_copy(half, half, fr_sem).wait()


def solution(mesh):
    dma, vmem, bf16 = pltpu.SemaphoreType.DMA, pltpu.VMEM, jnp.bfloat16
    anyspace = pl.BlockSpec(memory_space=pl.ANY)
    call = pl.pallas_call(
        kernel,
        out_shape=jax.ShapeDtypeStruct((N, D, FF), bf16),
        in_specs=[anyspace, anyspace],
        out_specs=anyspace,
        scratch_shapes=[
            vmem((NR, RB, TOK), bf16),
            vmem((2, TOK, RB), bf16),
            vmem((2, TOK, CB), bf16),
            vmem((QP, RB, CB), jnp.float32),
            vmem((QD, HB, CB), bf16),
            vmem((QD, HB, CB), bf16),
            vmem((QX, HB, CB), bf16),
            vmem((QX, HB, CB), bf16),
            vmem((QF, HB, CB), bf16),
            dma((2,)), dma((2,)), dma((QD,)), dma((QD,)), dma((QX,)), dma((QX,)),
            dma((QF,)), dma((QF,)), dma(()),
            pltpu.SemaphoreType.REGULAR, pltpu.SemaphoreType.REGULAR,
        ],
        compiler_params=pltpu.CompilerParams(
            collective_id=0, has_side_effects=True, vmem_limit_bytes=60 * 2**20),
        cost_estimate=pl.CostEstimate(
            flops=2 * N * TOK * D * FF, bytes_accessed=2 * N * (TOK * (D + FF) + D * FF),
            transcendentals=0),
    )

    def step(a, g):
        return call(a[0], g[0])

    return jax.shard_map(
        step, mesh=mesh, in_specs=(P(("rep", "dp")), P(("rep", "dp"))),
        out_specs=P("rep"), check_vma=False)
```

```python
import functools

import jax
import jax.numpy as jnp
from jax import lax
from jax.experimental import pallas as pl
from jax.experimental.pallas import tpu as pltpu
from jax.sharding import PartitionSpec as P


MESH = pl.DeviceIdType.MESH
N, TOK, D, FF = 4, 4096, 1280, 4096
RB, CB = 256, 512
HC = CB // 2
HB = RB // 2
NR, NC = D // RB, FF // CB
PIECES = N * NC * NR
TAILS = (13, 2)
LATE = PIECES - sum(TAILS) - 1
INSIDE = LATE
KT = 512
LAG = 24
QX = LAG + 2
QD = 4
QP = 3
QF = 4


GROUPS = tuple((PIECES - sum(TAILS[i:]), PIECES - sum(TAILS[i + 1:])) for i in range(len(TAILS)))
MOVES, REST = INSIDE // NR, INSIDE % NR
QM = 8


def when(cond):
    return pl.when(cond)


def where(k):
    q = k // NR
    return q // NC, lax.rem(k, NR), lax.rem(q, NC)


def kernel(a, g, res, own0, own1, own2, sib0, sib1, sib2, got0, at, abuf, gbuf, prod, dsend, drecv, xsend, xrecv, fin, lsend, lrecv, lsum,
           a_sem, g_sem, ds_sem, dr_sem, xs_sem, xr_sem, fl_sem, fs_sem, fr_sem,
           to_sem, ts_sem, tr_sem, late_sem, dfree, xfree):
    rep, me = lax.axis_index("rep"), lax.axis_index("dp")
    core = lax.rem(me, 2)
    sibling = (rep, me + 1 - 2 * core)
    partner = (rep, lax.rem(me + 2, 4))
    mine = pl.multiple_of(core * HB, HB)
    other = pl.multiple_of((1 - core) * HB, HB)

    def load_a(t):
        n, r = t // NR, lax.rem(t, NR)
        s = lax.rem(t, 2)
        cols = pl.ds(pl.multiple_of(r * RB, RB), RB)
        return pltpu.make_async_copy(a.at[n, :, cols], abuf.at[s], a_sem.at[s])

    def load_g(q, h):
        n, c = q // NC, lax.rem(q, NC)
        s = lax.rem(q, 2)
        cols = pl.ds(pl.multiple_of(c * CB + h * HC, HC), HC)
        return pltpu.make_async_copy(g.at[n, :, cols], gbuf.at[s, :, pl.ds(h * HC, HC)], g_sem.at[s, h])

    def across_cores(k):
        s = lax.rem(k, QD)
        return pltpu.make_async_remote_copy(
            dsend.at[s], drecv.at[s], ds_sem.at[s], dr_sem.at[s],
            device_id=sibling, device_id_type=MESH)

    def across_chips(k):
        s = lax.rem(k, QX)
        return pltpu.make_async_remote_copy(
            xsend.at[s], xrecv.at[s], xs_sem.at[s], xr_sem.at[s],
            device_id=partner, device_id_type=MESH)

    def place(k):
        n, r, c = where(k)
        rows = pl.ds(pl.multiple_of(r * RB + mine, HB), HB)
        cols = pl.ds(pl.multiple_of(c * CB, CB), CB)
        return res.at[n, rows, cols]

    def tail(k, group):
        own, sib = ((own1, sib1), (own2, sib2))[group]
        i = k - LATE - 1
        j = i - sum(TAILS[:group])
        src = xsend.at[lax.rem(k, QX)]
        return (
            pltpu.make_async_copy(src, own.at[j], to_sem.at[i]),
            pltpu.make_async_remote_copy(
                src, sib.at[j], ts_sem.at[i], tr_sem.at[group],
                device_id=sibling, device_id_type=MESH))

    def keep(k):
        s = lax.rem(k, QF)
        return pltpu.make_async_copy(fin.at[s], place(k), fl_sem.at[s])

    def share(k):
        s = lax.rem(k, QF)
        return pltpu.make_async_remote_copy(
            fin.at[s], place(k), fs_sem.at[s], fr_sem.at[k // (MOVES * NR)],
            device_id=sibling, device_id_type=MESH)

    late_partial = pltpu.make_async_remote_copy(
        lsend, lrecv, late_sem.at[0], late_sem.at[1], device_id=sibling, device_id_type=MESH)
    late_swap = pltpu.make_async_remote_copy(
        lsum, got0.at[0], late_sem.at[2], late_sem.at[3], device_id=partner, device_id_type=MESH)
    late_keep = pltpu.make_async_copy(lsum, own0.at[0], late_sem.at[4])
    late_share = pltpu.make_async_remote_copy(
        lsum, sib0.at[0], late_sem.at[5], late_sem.at[6], device_id=sibling, device_id_type=MESH)

    def multiply(k):
        q, r = k // NR, lax.rem(k, NR)
        n, c = q // NC, lax.rem(q, NC)
        gs = lax.rem(q, 2)

        @when(c == 0)
        def _():
            t = n * NR + r
            s = lax.rem(t, 2)
            load_a(t).wait()

            @pl.loop(0, TOK // KT)
            def _(i):
                toks = pl.ds(pl.multiple_of(i * KT, KT), KT)
                at[r, :, toks] = abuf[s, toks, :].T

            @when(t + 2 < N * NR)
            def _():
                load_a(t + 2).start()

        p = lax.rem(k, QP)

        @when(r == 0)
        def _():
            for h in range(2):
                load_g(q, h).wait()

            @when(k == 0)
            def _():
                for h in range(2):
                    load_g(1, h).start()

        prod[p] = jnp.dot(at[r], gbuf[gs], preferred_element_type=jnp.float32)

        @when((r == NR - 1) & (q + 2 < N * NC))
        def _():
            for h in range(2):
                load_g(q + 2, h).start()

        @when(k == LATE)
        def _():
            @when(core == 0)
            def _():
                lsend[...] = prod[p].astype(jnp.bfloat16)
                late_partial.start()

        @when(k != LATE)
        def _():
            s = lax.rem(k, QD)

            @when(k >= QD)
            def _():
                across_cores(k - QD).wait_send()

                @when(k != LATE + QD)
                def _():
                    pl.semaphore_wait(dfree, 1)

            dsend[s] = prod[p, pl.ds(other, HB)].astype(jnp.bfloat16)
            across_cores(k).start()

    def chip_sum(k):
        @when(k == LATE)
        def _():
            @when(core == 1)
            def _():
                late_partial.wait_recv()
                total = prod[lax.rem(k, QP)] + lrecv[...].astype(jnp.float32)
                lsum[...] = total.astype(jnp.bfloat16)
                late_swap.start()
                late_keep.start()
                late_share.start()

        @when(k != LATE)
        def _():
            own_sum(k)

    def own_sum(k):
        across_cores(k).wait_recv()
        total = prod[lax.rem(k, QP), pl.ds(mine, HB)] + drecv[lax.rem(k, QD)].astype(jnp.float32)
        xsend[lax.rem(k, QX)] = total.astype(jnp.bfloat16)

        @when((k + QD < PIECES) & (k + QD != LATE))
        def _():
            pl.semaphore_signal(dfree, inc=1, device_id=sibling, device_id_type=MESH)

        @when((k >= QX) & (k < INSIDE))
        def _():
            pl.semaphore_wait(xfree, 1)

        @when(k < INSIDE)
        def _():
            across_chips(k).start()

        for group, (lo, hi) in enumerate(GROUPS):
            @when((k >= lo) & (k < hi))
            def _():
                for copy in tail(k, group):
                    copy.start()

    def finish(k):
        across_chips(k).wait()

        @when(k >= QF)
        def _():
            keep(k - QF).wait()
            share(k - QF).wait_send()

        s = lax.rem(k, QX)
        total = xsend[s].astype(jnp.float32) + xrecv[s].astype(jnp.float32)
        fin[lax.rem(k, QF)] = total.astype(jnp.bfloat16)

        @when(k + QX < INSIDE)
        def _():
            pl.semaphore_signal(xfree, inc=1, device_id=partner, device_id_type=MESH)

        keep(k).start()
        share(k).start()

    load_a(0).start()
    load_g(0, 0).start()
    load_g(0, 1).start()
    load_a(1).start()
    barrier = pltpu.get_barrier_semaphore()
    for peer in (sibling, partner):
        pl.semaphore_signal(barrier, inc=1, device_id=peer, device_id_type=MESH)
    pl.semaphore_wait(barrier, 2)

    @pl.loop(0, INSIDE + LAG)
    def _(k):
        @when(k < PIECES)
        def _():
            multiply(k)

        @when((k != 1) & (k <= PIECES))
        def _():
            chip_sum(jnp.maximum(k - 1, 0))

        @when(k >= LAG)
        def _():
            finish(k - LAG)

    @pl.loop(PIECES - QD, PIECES)
    def _(k):
        across_cores(k).wait_send()

    @pl.loop(INSIDE - QF, INSIDE)
    def _(k):
        keep(k).wait()
        share(k).wait_send()

    for group, (lo, hi) in enumerate(GROUPS):
        @pl.loop(lo, hi)
        def _(k):
            own, sib = tail(k, group)
            own.wait()
            sib.wait_send()

        sib = (sib1, sib2)[group]
        pltpu.make_async_copy(sib, sib, tr_sem.at[group]).wait()

    whole = res.at[pl.ds(0, 2), :, pl.ds(0, MOVES * CB // 4)]
    pltpu.make_async_copy(whole, whole, fr_sem.at[0]).wait()
    rest = res.at[0, pl.ds(0, REST * HB), pl.ds(0, CB)]
    pltpu.make_async_copy(rest, rest, fr_sem.at[1]).wait()

    @when(core == 0)
    def _():
        late_partial.wait_send()
        late_share.wait_recv()

    @when(core == 1)
    def _():
        late_keep.wait()
        late_share.wait_send()
        late_swap.wait()


def move(res, out, buf, last, in_sem, out_sem, last_sem):
    def src(i):
        n, c = i // NC, lax.rem(i, NC)
        return n, slice(None), pl.ds(pl.multiple_of(c * CB, CB), CB)

    def load(i):
        s = lax.rem(i, QM)
        return pltpu.make_async_copy(res.at[src(i)], buf.at[s], in_sem.at[s])

    def store(i):
        s = lax.rem(i, QM)
        return pltpu.make_async_copy(buf.at[s], out.at[src(i)], out_sem.at[s])

    n, c = MOVES // NC, MOVES % NC
    block = (n, pl.ds(0, REST * RB), pl.ds(c * CB, CB))
    last_in = pltpu.make_async_copy(res.at[block], last, last_sem.at[0])
    last_out = pltpu.make_async_copy(last, out.at[block], last_sem.at[1])
    for i in range(QM):
        load(i).start()
    last_in.start()

    @pl.loop(0, MOVES)
    def _(i):
        load(i).wait()
        store(i).start()
        j = i - QM // 2

        @when((j >= 0) & (j + QM < MOVES))
        def _():
            store(j).wait()
            load(j + QM).start()

    last_in.wait()
    last_out.start()

    @pl.loop(MOVES - QM, MOVES)
    def _(i):
        store(i).wait()

    last_out.wait()


def settle_late(_, own, sib, got, lent, out, buf, sem):
    core = lax.rem(lax.axis_index("dp"), 2)
    n, r, c = LATE // NR // NC, LATE % NR, LATE // NR % NC
    for i, (mine, theirs) in enumerate(((sib, lent), (own, got))):
        @when(core == i)
        def _():
            total = mine[0].astype(jnp.float32) + theirs[0].astype(jnp.float32)
            buf[...] = total.astype(jnp.bfloat16)
    copy = pltpu.make_async_copy(buf, out.at[n, pl.ds(r * RB, RB), pl.ds(c * CB, CB)], sem)
    copy.start()
    copy.wait()


def settle(first, count, _, own, sib, got, lent, out, buf, sem):
    core = lax.rem(lax.axis_index("dp"), 2)
    pairs = ((core, own, got), (1 - core, sib, lent))

    def store(i, h):
        n, r, c = where(jnp.int32(first + i))
        rows = pl.ds(pl.multiple_of(r * RB + pairs[h][0] * HB, HB), HB)
        cols = pl.ds(pl.multiple_of(c * CB, CB), CB)
        return pltpu.make_async_copy(buf.at[h, i], out.at[n, rows, cols], sem.at[h, i])

    for i in range(count):
        for h, (_, mine, theirs) in enumerate(pairs):
            total = mine[i].astype(jnp.float32) + theirs[i].astype(jnp.float32)
            buf[h, i] = total.astype(jnp.bfloat16)
            store(i, h).start()
    for i in range(count):
        for h in range(2):
            store(i, h).wait()


def solution(mesh):
    dma, vmem, bf16 = pltpu.SemaphoreType.DMA, pltpu.VMEM, jnp.bfloat16
    anyspace = pl.BlockSpec(memory_space=pl.ANY)
    result = jax.ShapeDtypeStruct((N, D, FF), bf16)
    tails = [jax.ShapeDtypeStruct((t, HB, CB), bf16) for t in TAILS]
    late = jax.ShapeDtypeStruct((1, RB, CB), bf16)
    reduce = pl.pallas_call(
        kernel,
        out_shape=[result, late, *tails, late, *tails, late],
        in_specs=[anyspace, anyspace],
        out_specs=[anyspace] * 8,
        scratch_shapes=[
            vmem((NR, RB, TOK), bf16),
            vmem((2, TOK, RB), bf16),
            vmem((2, TOK, CB), bf16),
            vmem((QP, RB, CB), jnp.float32),
            vmem((QD, HB, CB), bf16),
            vmem((QD, HB, CB), bf16),
            vmem((QX, HB, CB), bf16),
            vmem((QX, HB, CB), bf16),
            vmem((QF, HB, CB), bf16),
            vmem((RB, CB), bf16), vmem((RB, CB), bf16), vmem((RB, CB), bf16),
            dma((2,)), dma((2, 2)), dma((QD,)), dma((QD,)), dma((QX,)), dma((QX,)),
            dma((QF,)), dma((QF,)), dma((2,)),
            dma((sum(TAILS),)), dma((sum(TAILS),)), dma((len(TAILS),)), dma((7,)),
            pltpu.SemaphoreType.REGULAR, pltpu.SemaphoreType.REGULAR,
        ],
        compiler_params=pltpu.CompilerParams(
            collective_id=0, has_side_effects=True, vmem_limit_bytes=60 * 2**20),
        cost_estimate=pl.CostEstimate(
            flops=2 * N * TOK * D * FF, bytes_accessed=2 * N * (TOK * (D + FF) + D * FF),
            transcendentals=0),
        name="reduce",
    )
    copy = pl.pallas_call(
        move,
        out_shape=result,
        in_specs=[anyspace],
        out_specs=anyspace,
        scratch_shapes=[
            vmem((QM, D, CB), bf16), vmem((REST * RB, CB), bf16),
            dma((QM,)), dma((QM,)), dma((2,))],
        compiler_params=pltpu.CompilerParams(vmem_limit_bytes=60 * 2**20),
        cost_estimate=pl.CostEstimate(flops=10**10, bytes_accessed=4 * N * D * FF, transcendentals=0),
        name="move",
    )

    def last(group, out, *parts):
        lo, hi = GROUPS[group]
        count = hi - lo
        return pl.pallas_call(
            functools.partial(settle, lo, count),
            out_shape=result,
            in_specs=[anyspace] + [pl.BlockSpec(memory_space=pltpu.VMEM)] * 4,
            out_specs=anyspace,
            input_output_aliases={0: 0},
            scratch_shapes=[vmem((2, count, HB, CB), bf16), dma((2, count))],
            compiler_params=pltpu.CompilerParams(vmem_limit_bytes=8 * 2**20),
            cost_estimate=pl.CostEstimate(flops=10**8, bytes_accessed=count * 2**20, transcendentals=0),
        )(out, *parts)

    def settle_first(out, *parts):
        return pl.pallas_call(
            settle_late,
            out_shape=result,
            in_specs=[anyspace] + [pl.BlockSpec(memory_space=pltpu.VMEM)] * 4,
            out_specs=anyspace,
            input_output_aliases={0: 0},
            scratch_shapes=[vmem((RB, CB), bf16), dma(())],
            compiler_params=pltpu.CompilerParams(vmem_limit_bytes=8 * 2**20),
            cost_estimate=pl.CostEstimate(flops=10**8, bytes_accessed=2**20, transcendentals=0),
            name="settle_late",
        )(out, *parts)

    swap_chips = [(i, (i + 2) % 4) for i in range(4)]
    swap_cores = [(i, i ^ 1) for i in range(4)]

    def step(a, g):
        res, own0, own1, own2, sib0, sib1, sib2, got0 = reduce(a[0], g[0])
        got1 = lax.ppermute(own1, "dp", swap_chips)
        got2 = lax.ppermute(own2, "dp", swap_chips)
        lent0 = lax.ppermute(got0, "dp", [(1, 0), (3, 2)])
        out = copy(res)
        out = settle_first(out, own0, sib0, got0, lent0)
        out, got1 = lax.optimization_barrier((out, got1))
        lent1 = lax.ppermute(got1, "dp", swap_cores)
        out = last(0, out, own1, sib1, got1, lent1)
        out, got2 = lax.optimization_barrier((out, got2))
        lent2 = lax.ppermute(got2, "dp", swap_cores)
        return last(1, out, own2, sib2, got2, lent2)

    return jax.shard_map(
        step, mesh=mesh, in_specs=(P(("rep", "dp")), P(("rep", "dp"))),
        out_specs=P("rep"), check_vma=False)
```

```python
import functools

import jax
import jax.numpy as jnp
from jax import lax
from jax.experimental import pallas as pl
from jax.experimental.pallas import tpu as pltpu
from jax.sharding import PartitionSpec as P


MESH = pl.DeviceIdType.MESH
N, TOK, D, FF = 4, 4096, 1280, 4096
RB, CB = 256, 512
HC = CB // 2
HB = RB // 2
NR, NC = D // RB, FF // CB
PIECES = N * NC * NR
TAILS = (8, 5, 2)
LATES = 2
INSIDE = PIECES - sum(TAILS) - LATES
AFTER = INSIDE + LATES
KT = 512
LAG = 24
QX = LAG + 2
QD = 4
QP = 3
QF = 4


GROUPS = tuple((PIECES - sum(TAILS[i:]), PIECES - sum(TAILS[i + 1:])) for i in range(len(TAILS)))
MOVES, REST = INSIDE // NR, INSIDE % NR
QM = 8


def when(cond):
    return pl.when(cond)


def where(k):
    q = k // NR
    return q // NC, lax.rem(k, NR), lax.rem(q, NC)


def kernel(a, g, res, own0, sib0, got0, *refs):
    n = len(TAILS)
    owns, sibs = refs[:n], refs[n:2 * n]
    (at, abuf, gbuf, prod, dsend, drecv, xsend, xrecv, fin, lsend, lrecv, lsum,
     a_sem, g_sem, ds_sem, dr_sem, xs_sem, xr_sem, fl_sem, fs_sem, fr_sem,
     to_sem, ts_sem, tr_sem, late_sem, early_sem, dfree, xfree) = refs[2 * n:]
    rep, me = lax.axis_index("rep"), lax.axis_index("dp")
    core = lax.rem(me, 2)
    sibling = (rep, me + 1 - 2 * core)
    partner = (rep, lax.rem(me + 2, 4))
    mine = pl.multiple_of(core * HB, HB)
    other = pl.multiple_of((1 - core) * HB, HB)

    def load_a(t):
        n, r = t // NR, lax.rem(t, NR)
        s = lax.rem(t, 2)
        cols = pl.ds(pl.multiple_of(r * RB, RB), RB)
        return pltpu.make_async_copy(a.at[n, :, cols], abuf.at[s], a_sem.at[s])

    def load_g(q, h):
        n, c = q // NC, lax.rem(q, NC)
        s = lax.rem(q, 2)
        cols = pl.ds(pl.multiple_of(c * CB + h * HC, HC), HC)
        return pltpu.make_async_copy(g.at[n, :, cols], gbuf.at[s, :, pl.ds(h * HC, HC)], g_sem.at[s, h])

    def across_cores(k):
        s = lax.rem(k, QD)
        return pltpu.make_async_remote_copy(
            dsend.at[s], drecv.at[s], ds_sem.at[s], dr_sem.at[s],
            device_id=sibling, device_id_type=MESH)

    def across_chips(k):
        s = lax.rem(k, QX)
        return pltpu.make_async_remote_copy(
            xsend.at[s], xrecv.at[s], xs_sem.at[s], xr_sem.at[s],
            device_id=partner, device_id_type=MESH)

    def place(k):
        n, r, c = where(k)
        rows = pl.ds(pl.multiple_of(r * RB + mine, HB), HB)
        cols = pl.ds(pl.multiple_of(c * CB, CB), CB)
        return res.at[n, rows, cols]

    def tail(k, group):
        i = k - AFTER
        j = i - sum(TAILS[:group])
        src = xsend.at[lax.rem(k, QX)]
        return (
            pltpu.make_async_copy(src, owns[group].at[j], to_sem.at[i]),
            pltpu.make_async_remote_copy(
                src, sibs[group].at[j], ts_sem.at[i], tr_sem.at[group],
                device_id=sibling, device_id_type=MESH))

    def keep(k):
        s = lax.rem(k, QF)
        return pltpu.make_async_copy(fin.at[s], place(k), fl_sem.at[s])

    def share(k):
        s = lax.rem(k, QF)
        return pltpu.make_async_remote_copy(
            fin.at[s], place(k), fs_sem.at[s], fr_sem.at[k // (MOVES * NR)],
            device_id=sibling, device_id_type=MESH)

    def late_partial(i):
        return pltpu.make_async_remote_copy(
            lsend.at[i], lrecv.at[i], late_sem.at[i, 0], late_sem.at[i, 1],
            device_id=sibling, device_id_type=MESH)

    def late_swap(i):
        return pltpu.make_async_remote_copy(
            lsum.at[i], got0.at[i], late_sem.at[i, 2], late_sem.at[i, 3],
            device_id=partner, device_id_type=MESH)

    def late_keep(i):
        return pltpu.make_async_copy(lsum.at[i], own0.at[i], late_sem.at[i, 4])

    def late_share(i):
        return pltpu.make_async_remote_copy(
            lsum.at[i], sib0.at[i], late_sem.at[i, 5], late_sem.at[i, 6],
            device_id=sibling, device_id_type=MESH)

    def is_late(k):
        return (k >= INSIDE) & (k < AFTER)

    def turn(t):
        s, r = lax.rem(t, 2), lax.rem(t, NR)

        @pl.loop(0, TOK // KT)
        def _(i):
            toks = pl.ds(pl.multiple_of(i * KT, KT), KT)
            at[r, :, toks] = abuf[s, toks, :].T

        @when(t + 2 < N * NR)
        def _():
            load_a(t + 2).start()

    def first_piece():
        def part(ref, h, rows=slice(None)):
            return ref.at[0, rows, pl.ds(h * HC, HC)]

        def partial(h):
            return pltpu.make_async_remote_copy(
                part(dsend, h), part(drecv, h), ds_sem.at[0], early_sem.at[h],
                device_id=sibling, device_id_type=MESH)

        def swap(h):
            return pltpu.make_async_remote_copy(
                part(xsend, h), part(xrecv, h), xs_sem.at[0], xr_sem.at[0],
                device_id=partner, device_id_type=MESH)

        load_a(0).wait()
        load_g(0, 1).start()
        load_a(1).start()
        turn(jnp.int32(0))
        for h in range(2):
            load_g(0, h).wait()
            part(prod, h)[...] = jnp.dot(
                at[0], part(gbuf, h)[...], preferred_element_type=jnp.float32)
            part(dsend, h)[...] = part(prod, h, pl.ds(other, HB))[...].astype(jnp.bfloat16)
            partial(h).start()
        for h in range(2):
            load_g(1, h).start()
        for h in range(2):
            partial(h).wait_recv()
            total = part(prod, h, pl.ds(mine, HB))[...] + part(drecv, h)[...].astype(jnp.float32)
            part(xsend, h)[...] = total.astype(jnp.bfloat16)
            swap(h).start()
        pl.semaphore_signal(dfree, inc=1, device_id=sibling, device_id_type=MESH)

    def first_sum(k):
        across_cores(k).wait_recv()
        total = prod[lax.rem(k, QP), pl.ds(mine, HB)] + drecv[lax.rem(k, QD)].astype(jnp.float32)
        xsend[k] = total.astype(jnp.bfloat16)
        pl.semaphore_signal(dfree, inc=1, device_id=sibling, device_id_type=MESH)
        across_chips(k).start()

    def multiply(k):
        q, r = k // NR, lax.rem(k, NR)
        n, c = q // NC, lax.rem(q, NC)
        gs = lax.rem(q, 2)

        @when(c == 0)
        def _():
            load_a(n * NR + r).wait()
            turn(n * NR + r)

        @when((k >= 2) & (k <= NR))
        def _():
            first_sum(k - 1)

        @when(r == 0)
        def _():
            for h in range(2):
                load_g(q, h).wait()

        p = lax.rem(k, QP)
        prod[p] = jnp.dot(at[r], gbuf[gs], preferred_element_type=jnp.float32)

        @when((r == NR - 1) & (q + 2 < N * NC))
        def _():
            for h in range(2):
                load_g(q + 2, h).start()

        @when(is_late(k) & (core == 0))
        def _():
            lsend[k - INSIDE] = prod[p].astype(jnp.bfloat16)
            late_partial(k - INSIDE).start()

        @when(~is_late(k))
        def _():
            s = lax.rem(k, QD)

            @when(k >= QD)
            def _():
                across_cores(k - QD).wait_send()

                @when(~is_late(k - QD))
                def _():
                    pl.semaphore_wait(dfree, 1)

            dsend[s] = prod[p, pl.ds(other, HB)].astype(jnp.bfloat16)
            across_cores(k).start()

    def chip_sum(k):
        @when(is_late(k) & (core == 1))
        def _():
            i = k - INSIDE
            late_partial(i).wait_recv()
            total = prod[lax.rem(k, QP)] + lrecv[i].astype(jnp.float32)
            lsum[i] = total.astype(jnp.bfloat16)
            late_swap(i).start()
            late_keep(i).start()
            late_share(i).start()

        @when(~is_late(k))
        def _():
            own_sum(k)

    def own_sum(k):
        across_cores(k).wait_recv()
        total = prod[lax.rem(k, QP), pl.ds(mine, HB)] + drecv[lax.rem(k, QD)].astype(jnp.float32)
        xsend[lax.rem(k, QX)] = total.astype(jnp.bfloat16)

        @when((k + QD < PIECES) & ~is_late(k + QD))
        def _():
            pl.semaphore_signal(dfree, inc=1, device_id=sibling, device_id_type=MESH)

        @when((k >= QX) & (k < INSIDE))
        def _():
            pl.semaphore_wait(xfree, 1)

        @when(k < INSIDE)
        def _():
            across_chips(k).start()

        for group, (lo, hi) in enumerate(GROUPS):
            @when((k >= lo) & (k < hi))
            def _():
                for copy in tail(k, group):
                    copy.start()

    def finish(k):
        across_chips(k).wait()

        @when(k >= QF)
        def _():
            keep(k - QF).wait()
            share(k - QF).wait_send()

        s = lax.rem(k, QX)
        total = xsend[s].astype(jnp.float32) + xrecv[s].astype(jnp.float32)
        fin[lax.rem(k, QF)] = total.astype(jnp.bfloat16)

        @when(k + QX < INSIDE)
        def _():
            pl.semaphore_signal(xfree, inc=1, device_id=partner, device_id_type=MESH)

        keep(k).start()
        share(k).start()

    load_a(0).start()
    load_g(0, 0).start()
    barrier = pltpu.get_barrier_semaphore()
    for peer in (sibling, partner):
        pl.semaphore_signal(barrier, inc=1, device_id=peer, device_id_type=MESH)
    pl.semaphore_wait(barrier, 2)

    first_piece()

    @pl.loop(1, INSIDE + LAG)
    def _(k):
        @when(k < PIECES)
        def _():
            multiply(k)

        @when((k > NR) & (k <= PIECES))
        def _():
            chip_sum(k - 1)

        @when(k >= LAG)
        def _():
            finish(k - LAG)

    @pl.loop(PIECES - QD, PIECES)
    def _(k):
        across_cores(k).wait_send()

    @pl.loop(INSIDE - QF, INSIDE)
    def _(k):
        keep(k).wait()
        share(k).wait_send()

    for group, (lo, hi) in enumerate(GROUPS):
        @pl.loop(lo, hi)
        def _(k):
            own, sib = tail(k, group)
            own.wait()
            sib.wait_send()

        sib = sibs[group]
        pltpu.make_async_copy(sib, sib, tr_sem.at[group]).wait()

    whole = res.at[pl.ds(0, 2), :, pl.ds(0, MOVES * CB // 4)]
    pltpu.make_async_copy(whole, whole, fr_sem.at[0]).wait()
    rest = res.at[0, pl.ds(0, REST * HB), pl.ds(0, CB)]
    pltpu.make_async_copy(rest, rest, fr_sem.at[1]).wait()

    @when(core == 0)
    def _():
        for i in range(LATES):
            late_partial(i).wait_send()
            late_share(i).wait_recv()

    @when(core == 1)
    def _():
        for i in range(LATES):
            late_keep(i).wait()
            late_share(i).wait_send()
            late_swap(i).wait()


def move(res, out, buf, last, in_sem, out_sem, last_sem):
    def src(i):
        n, c = i // NC, lax.rem(i, NC)
        return n, slice(None), pl.ds(pl.multiple_of(c * CB, CB), CB)

    def load(i):
        s = lax.rem(i, QM)
        return pltpu.make_async_copy(res.at[src(i)], buf.at[s], in_sem.at[s])

    def store(i):
        s = lax.rem(i, QM)
        return pltpu.make_async_copy(buf.at[s], out.at[src(i)], out_sem.at[s])

    n, c = MOVES // NC, MOVES % NC
    block = (n, pl.ds(0, REST * RB), pl.ds(c * CB, CB))
    last_in = pltpu.make_async_copy(res.at[block], last, last_sem.at[0])
    last_out = pltpu.make_async_copy(last, out.at[block], last_sem.at[1])
    for i in range(QM):
        load(i).start()
    last_in.start()

    @pl.loop(0, MOVES)
    def _(i):
        load(i).wait()
        store(i).start()
        j = i - QM // 2

        @when((j >= 0) & (j + QM < MOVES))
        def _():
            store(j).wait()
            load(j + QM).start()

    last_in.wait()
    last_out.start()

    @pl.loop(MOVES - QM, MOVES)
    def _(i):
        store(i).wait()

    last_out.wait()


def settle_late(_, own, sib, got, lent, out, buf, sem):
    core = lax.rem(lax.axis_index("dp"), 2)
    for i, (mine, theirs) in enumerate(((sib, lent), (own, got))):
        @when(core == i)
        def _():
            for j in range(LATES):
                total = mine[j].astype(jnp.float32) + theirs[j].astype(jnp.float32)
                buf[j] = total.astype(jnp.bfloat16)
    copies = []
    for j in range(LATES):
        n, r, c = where(jnp.int32(INSIDE + j))
        rows = pl.ds(pl.multiple_of(r * RB, RB), RB)
        cols = pl.ds(pl.multiple_of(c * CB, CB), CB)
        copies.append(pltpu.make_async_copy(buf.at[j], out.at[n, rows, cols], sem.at[j]))
    for copy in copies:
        copy.start()
    for copy in copies:
        copy.wait()


def settle(first, count, _, own, sib, got, lent, out, buf, sem):
    core = lax.rem(lax.axis_index("dp"), 2)
    pairs = ((core, own, got), (1 - core, sib, lent))

    def store(i, h):
        n, r, c = where(jnp.int32(first + i))
        rows = pl.ds(pl.multiple_of(r * RB + pairs[h][0] * HB, HB), HB)
        cols = pl.ds(pl.multiple_of(c * CB, CB), CB)
        return pltpu.make_async_copy(buf.at[h, i], out.at[n, rows, cols], sem.at[h, i])

    for i in range(count):
        for h, (_, mine, theirs) in enumerate(pairs):
            total = mine[i].astype(jnp.float32) + theirs[i].astype(jnp.float32)
            buf[h, i] = total.astype(jnp.bfloat16)
            store(i, h).start()
    for i in range(count):
        for h in range(2):
            store(i, h).wait()


def solution(mesh):
    dma, vmem, bf16 = pltpu.SemaphoreType.DMA, pltpu.VMEM, jnp.bfloat16
    anyspace = pl.BlockSpec(memory_space=pl.ANY)
    result = jax.ShapeDtypeStruct((N, D, FF), bf16)
    tails = [jax.ShapeDtypeStruct((t, HB, CB), bf16) for t in TAILS]
    late = jax.ShapeDtypeStruct((LATES, RB, CB), bf16)
    reduce = pl.pallas_call(
        kernel,
        out_shape=[result, late, late, late, *tails, *tails],
        in_specs=[anyspace, anyspace],
        out_specs=[anyspace] * (4 + 2 * len(TAILS)),
        scratch_shapes=[
            vmem((NR, RB, TOK), bf16),
            vmem((2, TOK, RB), bf16),
            vmem((2, TOK, CB), bf16),
            vmem((QP, RB, CB), jnp.float32),
            vmem((QD, HB, CB), bf16),
            vmem((QD, HB, CB), bf16),
            vmem((QX, HB, CB), bf16),
            vmem((QX, HB, CB), bf16),
            vmem((QF, HB, CB), bf16),
            *[vmem((LATES, RB, CB), bf16)] * 3,
            dma((2,)), dma((2, 2)), dma((QD,)), dma((QD,)), dma((QX,)), dma((QX,)),
            dma((QF,)), dma((QF,)), dma((2,)),
            dma((sum(TAILS),)), dma((sum(TAILS),)), dma((len(TAILS),)), dma((LATES, 7)), dma((2,)),
            pltpu.SemaphoreType.REGULAR, pltpu.SemaphoreType.REGULAR,
        ],
        compiler_params=pltpu.CompilerParams(
            collective_id=0, has_side_effects=True, vmem_limit_bytes=60 * 2**20),
        cost_estimate=pl.CostEstimate(
            flops=2 * N * TOK * D * FF, bytes_accessed=2 * N * (TOK * (D + FF) + D * FF),
            transcendentals=0),
        name="reduce",
    )
    copy = pl.pallas_call(
        move,
        out_shape=result,
        in_specs=[anyspace],
        out_specs=anyspace,
        scratch_shapes=[
            vmem((QM, D, CB), bf16), vmem((REST * RB, CB), bf16),
            dma((QM,)), dma((QM,)), dma((2,))],
        compiler_params=pltpu.CompilerParams(vmem_limit_bytes=60 * 2**20),
        cost_estimate=pl.CostEstimate(flops=10**10, bytes_accessed=4 * N * D * FF, transcendentals=0),
        name="move",
    )

    def last(group, out, *parts):
        lo, hi = GROUPS[group]
        count = hi - lo
        return pl.pallas_call(
            functools.partial(settle, lo, count),
            out_shape=result,
            in_specs=[anyspace] + [pl.BlockSpec(memory_space=pltpu.VMEM)] * 4,
            out_specs=anyspace,
            input_output_aliases={0: 0},
            scratch_shapes=[vmem((2, count, HB, CB), bf16), dma((2, count))],
            compiler_params=pltpu.CompilerParams(vmem_limit_bytes=8 * 2**20),
            cost_estimate=pl.CostEstimate(flops=10**8, bytes_accessed=count * 2**20, transcendentals=0),
        )(out, *parts)

    def settle_first(out, *parts):
        return pl.pallas_call(
            settle_late,
            out_shape=result,
            in_specs=[anyspace] + [pl.BlockSpec(memory_space=pltpu.VMEM)] * 4,
            out_specs=anyspace,
            input_output_aliases={0: 0},
            scratch_shapes=[vmem((LATES, RB, CB), bf16), dma((LATES,))],
            compiler_params=pltpu.CompilerParams(vmem_limit_bytes=8 * 2**20),
            cost_estimate=pl.CostEstimate(flops=10**8, bytes_accessed=2**20, transcendentals=0),
            name="settle_late",
        )(out, *parts)

    swap_chips = [(i, (i + 2) % 4) for i in range(4)]
    swap_cores = [(i, i ^ 1) for i in range(4)]

    def step(a, g):
        res, own0, sib0, got0, *tail = reduce(a[0], g[0])
        owns, sibs = tail[:len(TAILS)], tail[len(TAILS):]
        gots = []
        for own in owns:
            gots.append(lax.ppermute(own, "dp", swap_chips))
        lent0 = lax.ppermute(got0, "dp", [(1, 0), (3, 2)])
        out = copy(res)
        out = settle_first(out, own0, sib0, got0, lent0)
        for i, (own, sib, got) in enumerate(zip(owns, sibs, gots)):
            out, got = lax.optimization_barrier((out, got))
            lent = lax.ppermute(got, "dp", swap_cores)
            out = last(i, out, own, sib, got, lent)
        return out

    return jax.shard_map(
        step, mesh=mesh, in_specs=(P(("rep", "dp")), P(("rep", "dp"))),
        out_specs=P("rep"), check_vma=False)
```

```python
import functools

import jax
import jax.numpy as jnp
from jax import lax
from jax.experimental import pallas as pl
from jax.experimental.pallas import tpu as pltpu
from jax.sharding import PartitionSpec as P


MESH = pl.DeviceIdType.MESH
N, TOK, D, FF = 4, 4096, 1280, 4096
RB, CB = 256, 512
HC = CB // 2
HB = RB // 2
NR, NC = D // RB, FF // CB
PIECES = N * NC * NR
TAILS = (8, 5, 2)
LATES = 2
INSIDE = PIECES - sum(TAILS) - LATES
AFTER = INSIDE + LATES
KT = 512
LAG = 24
QX = LAG + 2
QD = 4
QP = 3
FIRST = 1
QF = 4


GROUPS = tuple((PIECES - sum(TAILS[i:]), PIECES - sum(TAILS[i + 1:])) for i in range(len(TAILS)))
MOVES, REST = INSIDE // NR, INSIDE % NR
QM = 8


def when(cond):
    return pl.when(cond)


def where(k):
    q = k // NR
    return q // NC, lax.rem(k, NR), lax.rem(q, NC)


def kernel(a, g, res, own0, sib0, got0, *refs):
    n = len(TAILS)
    owns, sibs = refs[:n], refs[n:2 * n]
    (at, abuf, gbuf, prod, dsend, drecv, xsend, xrecv, fin, lsend, lrecv, lsum,
     a_sem, g_sem, ds_sem, dr_sem, xs_sem, xr_sem, fl_sem, fs_sem, fr_sem,
     to_sem, ts_sem, tr_sem, late_sem, early_sem, dfree, xfree) = refs[2 * n:]
    rep, me = lax.axis_index("rep"), lax.axis_index("dp")
    core = lax.rem(me, 2)
    sibling = (rep, me + 1 - 2 * core)
    partner = (rep, lax.rem(me + 2, 4))
    mine = pl.multiple_of(core * HB, HB)
    other = pl.multiple_of((1 - core) * HB, HB)

    def load_a(t):
        n, r = t // NR, lax.rem(t, NR)
        s = lax.rem(t, 2)
        cols = pl.ds(pl.multiple_of(r * RB, RB), RB)
        return pltpu.make_async_copy(a.at[n, :, cols], abuf.at[s], a_sem.at[s])

    def load_g(q, h):
        n, c = q // NC, lax.rem(q, NC)
        s = lax.rem(q, 2)
        cols = pl.ds(pl.multiple_of(c * CB + h * HC, HC), HC)
        return pltpu.make_async_copy(g.at[n, :, cols], gbuf.at[s, :, pl.ds(h * HC, HC)], g_sem.at[s, h])

    def across_cores(k):
        s = lax.rem(k, QD)
        return pltpu.make_async_remote_copy(
            dsend.at[s], drecv.at[s], ds_sem.at[s], dr_sem.at[s],
            device_id=sibling, device_id_type=MESH)

    def across_chips(k):
        s = lax.rem(k, QX)
        return pltpu.make_async_remote_copy(
            xsend.at[s], xrecv.at[s], xs_sem.at[s], xr_sem.at[s],
            device_id=partner, device_id_type=MESH)

    def place(k):
        n, r, c = where(k)
        rows = pl.ds(pl.multiple_of(r * RB + mine, HB), HB)
        cols = pl.ds(pl.multiple_of(c * CB, CB), CB)
        return res.at[n, rows, cols]

    def tail(k, group):
        i = k - AFTER
        j = i - sum(TAILS[:group])
        src = xsend.at[lax.rem(k, QX)]
        return (
            pltpu.make_async_copy(src, owns[group].at[j], to_sem.at[i]),
            pltpu.make_async_remote_copy(
                src, sibs[group].at[j], ts_sem.at[i], tr_sem.at[group],
                device_id=sibling, device_id_type=MESH))

    def keep(k):
        s = lax.rem(k, QF)
        return pltpu.make_async_copy(fin.at[s], place(k), fl_sem.at[s])

    def share(k):
        s = lax.rem(k, QF)
        return pltpu.make_async_remote_copy(
            fin.at[s], place(k), fs_sem.at[s], fr_sem.at[k // (MOVES * NR)],
            device_id=sibling, device_id_type=MESH)

    def late_partial(i):
        return pltpu.make_async_remote_copy(
            lsend.at[i], lrecv.at[i], late_sem.at[i, 0], late_sem.at[i, 1],
            device_id=sibling, device_id_type=MESH)

    def late_swap(i):
        return pltpu.make_async_remote_copy(
            lsum.at[i], got0.at[i], late_sem.at[i, 2], late_sem.at[i, 3],
            device_id=partner, device_id_type=MESH)

    def late_keep(i):
        return pltpu.make_async_copy(lsum.at[i], own0.at[i], late_sem.at[i, 4])

    def late_share(i):
        return pltpu.make_async_remote_copy(
            lsum.at[i], sib0.at[i], late_sem.at[i, 5], late_sem.at[i, 6],
            device_id=sibling, device_id_type=MESH)

    def is_late(k):
        return (k >= INSIDE) & (k < AFTER)

    def turn(t):
        s, r = lax.rem(t, 2), lax.rem(t, NR)

        @pl.loop(0, TOK // KT)
        def _(i):
            toks = pl.ds(pl.multiple_of(i * KT, KT), KT)
            at[r, :, toks] = abuf[s, toks, :].T

        @when(t + 2 < N * NR)
        def _():
            load_a(t + 2).start()

    def first_piece(k):
        def part(ref, h, rows=slice(None), slot=k):
            return ref.at[slot, rows, pl.ds(h * HC, HC)]

        def partial(h):
            return pltpu.make_async_remote_copy(
                part(dsend, h), part(drecv, h), ds_sem.at[k], early_sem.at[k, h],
                device_id=sibling, device_id_type=MESH)

        def swap(h):
            return pltpu.make_async_remote_copy(
                part(xsend, h), part(xrecv, h), xs_sem.at[k], xr_sem.at[k],
                device_id=partner, device_id_type=MESH)

        for h in range(2):
            if k == 0:
                load_g(0, h).wait()
            part(prod, h)[...] = jnp.dot(
                at[k], part(gbuf, h, slot=0)[...], preferred_element_type=jnp.float32)
            part(dsend, h)[...] = part(prod, h, pl.ds(other, HB))[...].astype(jnp.bfloat16)
            partial(h).start()
        load_a(k + 1).wait()
        turn(jnp.int32(k + 1))
        if k == 0:
            for h in range(2):
                load_g(1, h).start()
        for h in range(2):
            partial(h).wait_recv()
            total = part(prod, h, pl.ds(mine, HB))[...] + part(drecv, h)[...].astype(jnp.float32)
            part(xsend, h)[...] = total.astype(jnp.bfloat16)
            swap(h).start()
        pl.semaphore_signal(dfree, inc=1, device_id=sibling, device_id_type=MESH)

    def first_sum(k):
        across_cores(k).wait_recv()
        total = prod[lax.rem(k, QP), pl.ds(mine, HB)] + drecv[lax.rem(k, QD)].astype(jnp.float32)
        xsend[k] = total.astype(jnp.bfloat16)
        pl.semaphore_signal(dfree, inc=1, device_id=sibling, device_id_type=MESH)
        across_chips(k).start()

    def multiply(k):
        q, r = k // NR, lax.rem(k, NR)
        n, c = q // NC, lax.rem(q, NC)
        gs = lax.rem(q, 2)

        @when((c == 0) & (k > FIRST))
        def _():
            load_a(n * NR + r).wait()
            turn(n * NR + r)

        @when((k > FIRST) & (k <= NR))
        def _():
            first_sum(k - 1)

        @when(r == 0)
        def _():
            for h in range(2):
                load_g(q, h).wait()

        p = lax.rem(k, QP)
        prod[p] = jnp.dot(at[r], gbuf[gs], preferred_element_type=jnp.float32)

        @when((r == NR - 1) & (q + 2 < N * NC))
        def _():
            for h in range(2):
                load_g(q + 2, h).start()

        @when(is_late(k) & (core == 0))
        def _():
            lsend[k - INSIDE] = prod[p].astype(jnp.bfloat16)
            late_partial(k - INSIDE).start()

        @when(~is_late(k))
        def _():
            s = lax.rem(k, QD)

            @when(k >= QD)
            def _():
                across_cores(k - QD).wait_send()

                @when(~is_late(k - QD))
                def _():
                    pl.semaphore_wait(dfree, 1)

            dsend[s] = prod[p, pl.ds(other, HB)].astype(jnp.bfloat16)
            across_cores(k).start()

    def chip_sum(k):
        @when(is_late(k) & (core == 1))
        def _():
            i = k - INSIDE
            late_partial(i).wait_recv()
            total = prod[lax.rem(k, QP)] + lrecv[i].astype(jnp.float32)
            lsum[i] = total.astype(jnp.bfloat16)
            late_swap(i).start()
            late_keep(i).start()
            late_share(i).start()

        @when(~is_late(k))
        def _():
            own_sum(k)

    def own_sum(k):
        across_cores(k).wait_recv()
        total = prod[lax.rem(k, QP), pl.ds(mine, HB)] + drecv[lax.rem(k, QD)].astype(jnp.float32)
        xsend[lax.rem(k, QX)] = total.astype(jnp.bfloat16)

        @when((k + QD < PIECES) & ~is_late(k + QD))
        def _():
            pl.semaphore_signal(dfree, inc=1, device_id=sibling, device_id_type=MESH)

        @when((k >= QX) & (k < INSIDE))
        def _():
            pl.semaphore_wait(xfree, 1)

        @when(k < INSIDE)
        def _():
            across_chips(k).start()

        for group, (lo, hi) in enumerate(GROUPS):
            @when((k >= lo) & (k < hi))
            def _():
                for copy in tail(k, group):
                    copy.start()

    def finish(k):
        across_chips(k).wait()

        @when(k >= QF)
        def _():
            keep(k - QF).wait()
            share(k - QF).wait_send()

        s = lax.rem(k, QX)
        total = xsend[s].astype(jnp.float32) + xrecv[s].astype(jnp.float32)
        fin[lax.rem(k, QF)] = total.astype(jnp.bfloat16)

        @when(k + QX < INSIDE)
        def _():
            pl.semaphore_signal(xfree, inc=1, device_id=partner, device_id_type=MESH)

        keep(k).start()
        share(k).start()

    load_a(0).start()
    load_g(0, 0).start()
    barrier = pltpu.get_barrier_semaphore()
    for peer in (sibling, partner):
        pl.semaphore_signal(barrier, inc=1, device_id=peer, device_id_type=MESH)
    pl.semaphore_wait(barrier, 2)

    load_a(0).wait()
    load_g(0, 1).start()
    load_a(1).start()
    turn(jnp.int32(0))
    for k in range(FIRST):
        first_piece(k)

    @pl.loop(FIRST, INSIDE + LAG)
    def _(k):
        @when(k < PIECES)
        def _():
            multiply(k)

        @when((k > NR) & (k <= PIECES))
        def _():
            chip_sum(k - 1)

        @when(k >= LAG)
        def _():
            finish(k - LAG)

    @pl.loop(PIECES - QD, PIECES)
    def _(k):
        across_cores(k).wait_send()

    @pl.loop(INSIDE - QF, INSIDE)
    def _(k):
        keep(k).wait()
        share(k).wait_send()

    for group, (lo, hi) in enumerate(GROUPS):
        @pl.loop(lo, hi)
        def _(k):
            own, sib = tail(k, group)
            own.wait()
            sib.wait_send()

        sib = sibs[group]
        pltpu.make_async_copy(sib, sib, tr_sem.at[group]).wait()

    whole = res.at[pl.ds(0, 2), :, pl.ds(0, MOVES * CB // 4)]
    pltpu.make_async_copy(whole, whole, fr_sem.at[0]).wait()
    rest = res.at[0, pl.ds(0, REST * HB), pl.ds(0, CB)]
    pltpu.make_async_copy(rest, rest, fr_sem.at[1]).wait()

    @when(core == 0)
    def _():
        for i in range(LATES):
            late_partial(i).wait_send()
            late_share(i).wait_recv()

    @when(core == 1)
    def _():
        for i in range(LATES):
            late_keep(i).wait()
            late_share(i).wait_send()
            late_swap(i).wait()


def move(res, out, buf, last, in_sem, out_sem, last_sem):
    def src(i):
        n, c = i // NC, lax.rem(i, NC)
        return n, slice(None), pl.ds(pl.multiple_of(c * CB, CB), CB)

    def load(i):
        s = lax.rem(i, QM)
        return pltpu.make_async_copy(res.at[src(i)], buf.at[s], in_sem.at[s])

    def store(i):
        s = lax.rem(i, QM)
        return pltpu.make_async_copy(buf.at[s], out.at[src(i)], out_sem.at[s])

    n, c = MOVES // NC, MOVES % NC
    block = (n, pl.ds(0, REST * RB), pl.ds(c * CB, CB))
    last_in = pltpu.make_async_copy(res.at[block], last, last_sem.at[0])
    last_out = pltpu.make_async_copy(last, out.at[block], last_sem.at[1])
    for i in range(QM):
        load(i).start()
    last_in.start()

    @pl.loop(0, MOVES)
    def _(i):
        load(i).wait()
        store(i).start()
        j = i - QM // 2

        @when((j >= 0) & (j + QM < MOVES))
        def _():
            store(j).wait()
            load(j + QM).start()

    last_in.wait()
    last_out.start()

    @pl.loop(MOVES - QM, MOVES)
    def _(i):
        store(i).wait()

    last_out.wait()


def settle_late(_, own, sib, got, lent, out, buf, sem):
    core = lax.rem(lax.axis_index("dp"), 2)
    for i, (mine, theirs) in enumerate(((sib, lent), (own, got))):
        @when(core == i)
        def _():
            for j in range(LATES):
                total = mine[j].astype(jnp.float32) + theirs[j].astype(jnp.float32)
                buf[j] = total.astype(jnp.bfloat16)
    copies = []
    for j in range(LATES):
        n, r, c = where(jnp.int32(INSIDE + j))
        rows = pl.ds(pl.multiple_of(r * RB, RB), RB)
        cols = pl.ds(pl.multiple_of(c * CB, CB), CB)
        copies.append(pltpu.make_async_copy(buf.at[j], out.at[n, rows, cols], sem.at[j]))
    for copy in copies:
        copy.start()
    for copy in copies:
        copy.wait()


def settle(first, count, _, own, sib, got, lent, out, buf, sem):
    core = lax.rem(lax.axis_index("dp"), 2)
    pairs = ((core, own, got), (1 - core, sib, lent))

    def store(i, h):
        n, r, c = where(jnp.int32(first + i))
        rows = pl.ds(pl.multiple_of(r * RB + pairs[h][0] * HB, HB), HB)
        cols = pl.ds(pl.multiple_of(c * CB, CB), CB)
        return pltpu.make_async_copy(buf.at[h, i], out.at[n, rows, cols], sem.at[h, i])

    for i in range(count):
        for h, (_, mine, theirs) in enumerate(pairs):
            total = mine[i].astype(jnp.float32) + theirs[i].astype(jnp.float32)
            buf[h, i] = total.astype(jnp.bfloat16)
            store(i, h).start()
    for i in range(count):
        for h in range(2):
            store(i, h).wait()


def solution(mesh):
    dma, vmem, bf16 = pltpu.SemaphoreType.DMA, pltpu.VMEM, jnp.bfloat16
    anyspace = pl.BlockSpec(memory_space=pl.ANY)
    result = jax.ShapeDtypeStruct((N, D, FF), bf16)
    tails = [jax.ShapeDtypeStruct((t, HB, CB), bf16) for t in TAILS]
    late = jax.ShapeDtypeStruct((LATES, RB, CB), bf16)
    reduce = pl.pallas_call(
        kernel,
        out_shape=[result, late, late, late, *tails, *tails],
        in_specs=[anyspace, anyspace],
        out_specs=[anyspace] * (4 + 2 * len(TAILS)),
        scratch_shapes=[
            vmem((NR, RB, TOK), bf16),
            vmem((2, TOK, RB), bf16),
            vmem((2, TOK, CB), bf16),
            vmem((QP, RB, CB), jnp.float32),
            vmem((QD, HB, CB), bf16),
            vmem((QD, HB, CB), bf16),
            vmem((QX, HB, CB), bf16),
            vmem((QX, HB, CB), bf16),
            vmem((QF, HB, CB), bf16),
            *[vmem((LATES, RB, CB), bf16)] * 3,
            dma((2,)), dma((2, 2)), dma((QD,)), dma((QD,)), dma((QX,)), dma((QX,)),
            dma((QF,)), dma((QF,)), dma((2,)),
            dma((sum(TAILS),)), dma((sum(TAILS),)), dma((len(TAILS),)), dma((LATES, 7)), dma((FIRST, 2)),
            pltpu.SemaphoreType.REGULAR, pltpu.SemaphoreType.REGULAR,
        ],
        compiler_params=pltpu.CompilerParams(
            collective_id=0, has_side_effects=True, vmem_limit_bytes=60 * 2**20),
        cost_estimate=pl.CostEstimate(
            flops=2 * N * TOK * D * FF, bytes_accessed=2 * N * (TOK * (D + FF) + D * FF),
            transcendentals=0),
        name="reduce",
    )
    copy = pl.pallas_call(
        move,
        out_shape=result,
        in_specs=[anyspace],
        out_specs=anyspace,
        scratch_shapes=[
            vmem((QM, D, CB), bf16), vmem((REST * RB, CB), bf16),
            dma((QM,)), dma((QM,)), dma((2,))],
        compiler_params=pltpu.CompilerParams(vmem_limit_bytes=60 * 2**20),
        cost_estimate=pl.CostEstimate(flops=10**10, bytes_accessed=4 * N * D * FF, transcendentals=0),
        name="move",
    )

    def last(group, out, *parts):
        lo, hi = GROUPS[group]
        count = hi - lo
        return pl.pallas_call(
            functools.partial(settle, lo, count),
            out_shape=result,
            in_specs=[anyspace] + [pl.BlockSpec(memory_space=pltpu.VMEM)] * 4,
            out_specs=anyspace,
            input_output_aliases={0: 0},
            scratch_shapes=[vmem((2, count, HB, CB), bf16), dma((2, count))],
            compiler_params=pltpu.CompilerParams(vmem_limit_bytes=8 * 2**20),
            cost_estimate=pl.CostEstimate(flops=10**8, bytes_accessed=count * 2**20, transcendentals=0),
        )(out, *parts)

    def settle_first(out, *parts):
        return pl.pallas_call(
            settle_late,
            out_shape=result,
            in_specs=[anyspace] + [pl.BlockSpec(memory_space=pltpu.VMEM)] * 4,
            out_specs=anyspace,
            input_output_aliases={0: 0},
            scratch_shapes=[vmem((LATES, RB, CB), bf16), dma((LATES,))],
            compiler_params=pltpu.CompilerParams(vmem_limit_bytes=8 * 2**20),
            cost_estimate=pl.CostEstimate(flops=10**8, bytes_accessed=2**20, transcendentals=0),
            name="settle_late",
        )(out, *parts)

    swap_chips = [(i, (i + 2) % 4) for i in range(4)]
    swap_cores = [(i, i ^ 1) for i in range(4)]

    def step(a, g):
        res, own0, sib0, got0, *tail = reduce(a[0], g[0])
        owns, sibs = tail[:len(TAILS)], tail[len(TAILS):]
        gots = []
        for own in owns:
            gots.append(lax.ppermute(own, "dp", swap_chips))
        lent0 = lax.ppermute(got0, "dp", [(1, 0), (3, 2)])
        out = copy(res)
        out = settle_first(out, own0, sib0, got0, lent0)
        for i, (own, sib, got) in enumerate(zip(owns, sibs, gots)):
            out, got = lax.optimization_barrier((out, got))
            lent = lax.ppermute(got, "dp", swap_cores)
            out = last(i, out, own, sib, got, lent)
        return out

    return jax.shard_map(
        step, mesh=mesh, in_specs=(P(("rep", "dp")), P(("rep", "dp"))),
        out_specs=P("rep"), check_vma=False)
```
